32 devices in a mesh: rep: 1 (over z), r: 4 (over y), s: 8 (over x, core).
Axes of the slice: x: 4, y: 4, z: 1, core: 2. Of those that a mesh axis runs over, the one named last changes fastest.
The devices are a block of a 4x4x8 slice.
Arguments:
- x: bfloat16 [32, 2048, 1024], P(('rep', 'r', 's'))
- dy: bfloat16 [32, 2048, 1024], P(('rep', 'r', 's'))
- w_gate: bfloat16 [2, 1024, 3328], P(None, 's')
- w_up: bfloat16 [2, 1024, 3328], P(None, 's')
- w_down: bfloat16 [2, 3328, 1024], P(None, 's')
- m_w_gate: float32 [2, 1024, 3328], P(None, 's')
- m_w_up: float32 [2, 1024, 3328], P(None, 's')
- m_w_down: float32 [2, 3328, 1024], P(None, 's')
- v_w_gate: float32 [2, 1024, 3328], P(None, 's')
- v_w_up: float32 [2, 1024, 3328], P(None, 's')
- v_w_down: float32 [2, 3328, 1024], P(None, 's')
Outputs:
- output 1: bfloat16 [2, 1024, 3328], P('rep', 's')
- output 2: bfloat16 [2, 1024, 3328], P('rep', 's')
- output 3: bfloat16 [2, 3328, 1024], P('rep', 's')
- output 4: float32 [2, 1024, 3328], P('rep', 's')
- output 5: float32 [2, 1024, 3328], P('rep', 's')
- output 6: float32 [2, 3328, 1024], P('rep', 's')
- output 7: float32 [2, 1024, 3328], P('rep', 's')
- output 8: float32 [2, 1024, 3328], P('rep', 's')
- output 9: float32 [2, 3328, 1024], P('rep', 's')
All inputs are finite; a program needn't handle non-finite values.
Results may differ from the reference program's by a relative error of at most 0.022.
Values are sent between devices in bfloat16 or wider.
A program may use at most 768 MiB of HBM per device.

```python
import jax
import jax.numpy as jnp
from jax import lax

SEQUENCES = 32
TOKENS = 2048
D = 1024
FF = 3328
LAYERS = 2
NAMES = ("w_gate", "w_up", "w_down")
SHAPES = {"w_gate": (LAYERS, D, FF), "w_up": (LAYERS, D, FF), "w_down": (LAYERS, FF, D)}


def bump(key, n, height):
    away = (jnp.arange(n, dtype=jnp.int32) - jax.random.randint(key, (), 0, n, jnp.int32)) % n
    return jnp.where(away < n // 8, height, 1.0)


def together(key, own, strength):
    shared = jax.random.normal(key, own.shape[1:], jnp.float32)
    return (own + strength * shared) * lax.rsqrt(1 + strength * strength)


def setup_inputs(seed: int = 0, part: int = 0) -> dict:
    kx, kdy, ka, kb, kz, kf, kh, kl, *keys = jax.random.split(jax.random.key(seed), 8 + 3 * len(NAMES))
    kx, kdy, ka, kb = (jax.random.fold_in(k, part) for k in (kx, kdy, ka, kb))
    kw, km, kv = (keys[i::3] for i in range(3))
    shape = (SEQUENCES, TOKENS, D)
    much_x, much_dy = jax.random.uniform(kz, (2,), jnp.float32, 0.0, 1.0)
    loud = 2.0 ** jax.random.uniform(jax.random.fold_in(kz, 1), (), jnp.float32, -1.0, 2.0)
    layers = 2.0 ** jax.random.uniform(kl, (LAYERS, 1, 1), jnp.float32, -1.0, 1.0)
    x = together(ka, jax.random.normal(kx, shape, jnp.float32), much_x) * bump(kf, D, 4.0)
    dy = together(kb, jax.random.normal(kdy, shape, jnp.float32), much_dy)
    drawn = {"x": x.astype(jnp.bfloat16), "dy": (loud * dy * (SEQUENCES * TOKENS) ** -0.5).astype(jnp.bfloat16)}
    for key, name in zip(kw, NAMES, strict=True):
        w = jax.random.normal(key, SHAPES[name], jnp.float32) * SHAPES[name][1] ** -0.5
        drawn[name] = (w * {"w_gate": 1.0, "w_up": bump(kh, FF, 4.0), "w_down": layers}[name]).astype(jnp.bfloat16)
    for key, name in zip(km, NAMES, strict=True):
        drawn[f"m_{name}"] = 0.1 * jax.random.normal(key, SHAPES[name], jnp.float32)
    for key, name in zip(kv, NAMES, strict=True):
        drawn[f"v_{name}"] = jax.random.uniform(key, SHAPES[name], jnp.float32, 0.005, 0.015)
    return drawn


def matmul(a, w):
    return jnp.dot(a, w, preferred_element_type=jnp.float32).astype(jnp.bfloat16)


def normed(h):
    wide = h.astype(jnp.float32)
    scale = lax.rsqrt(jnp.mean(wide**2, -1, keepdims=True) + 1e-6)
    return (wide * scale).astype(jnp.bfloat16)


def layer(h, w):
    a = normed(h)
    gate = jnp.dot(a, w["w_gate"], preferred_element_type=jnp.float32)
    up = jnp.dot(a, w["w_up"], preferred_element_type=jnp.float32)
    return h + matmul((jax.nn.silu(gate) * up).astype(jnp.bfloat16), w["w_down"])


def adamw(w, m, v, g):
    m = 0.9 * m + 0.1 * g
    v = 0.95 * v + 0.05 * g * g
    step = m * lax.rsqrt(v + 1e-8) + 0.1 * w
    return (w - 0.02 * step).astype(jnp.bfloat16), m, v


def stack(weights, h):
    return lax.scan(lambda h, w: (layer(h, w), None), h, weights)[0]


def reference(x, dy, w_gate, w_up, w_down, m_w_gate, m_w_up, m_w_down, v_w_gate, v_w_up, v_w_down):
    weights = dict(zip(NAMES, (w_gate, w_up, w_down), strict=True))

    def take(so_far, sequence):
        h, by_y = sequence
        _, back = jax.vjp(lambda w: stack(w, h), weights)
        return jax.tree.map(lambda total, term: total + term.astype(jnp.float32), so_far, back(by_y)[0]), None

    none_yet = {name: jnp.zeros(w.shape, jnp.float32) for name, w in weights.items()}
    by_weights, _ = lax.scan(take, none_yet, (x, dy))
    gradients = [by_weights[name].astype(jnp.bfloat16).astype(jnp.float32) for name in NAMES]
    new = [
        adamw(w.astype(jnp.float32), m, v, g)
        for w, m, v, g in zip((w_gate, w_up, w_down), (m_w_gate, m_w_up, m_w_down), (v_w_gate, v_w_up, v_w_down), gradients, strict=True)
    ]
    return tuple(one[which] for which in range(3) for one in new)
```

```python
import functools
import jax
import jax.numpy as jnp
from jax import lax
from jax.experimental import pallas as pl
from jax.experimental.pallas import tpu as pltpu
from jax.sharding import PartitionSpec as P

bf16, f32 = jnp.bfloat16, jnp.float32
C = 256
W = C + C
R = 256
MESH = pl.DeviceIdType.MESH
NN, NT = ((1,), (0,)), ((1,), (1,))


def dot(a, b, dims):
    return lax.dot_general(a, b, (dims, ((), ())), preferred_element_type=f32)


def ds(i, n):
    return pl.ds(pl.multiple_of(i * n, n), n)


def loop(first, last, f):
    def body(i, _):
        f(i)
        return 0
    lax.fori_loop(first, last, body, 0)


def place():
    z, y, s = (lax.axis_index(n) for n in ("rep", "r", "s"))
    x, c = s // 2, s % 2

    def pair(i):
        near, far = i + 1 - 2 * (i % 2), 3 - i
        return (1 - c) * near + c * far, c * near + (1 - c) * far

    return z, y, x, c, pair(x), pair(y)


def barrier(z, y, x, c, xs):
    sem = pltpu.get_barrier_semaphore()
    others = [(z, y, 2 * x + 1 - c)] + [(z, y, 2 * p + c) for p in xs] + [(z, (y + d) % 4, 2 * x + c) for d in (1, 3)]
    for o in others:
        pl.semaphore_signal(sem, inc=1, device_id=o, device_id_type=MESH)
    pl.semaphore_wait(sem, len(others))


class Gather:
    def __init__(self, where, own, full, block, width, sems):
        self.z, self.y, self.x, self.c, (self.p1, self.p2), _ = where
        self.own, self.full, self.block, self.width = own, full, block, width
        self.a, self.b1, self.b2, self.ys, self.e, self.s = sems
        self.opp = (self.x + 2) % 4
        self.o = 1 - self.c
        self.par = self.y % 2

    def dev(self, x=None, y=None, c=None):
        x, y, c = (self.x if x is None else x), (self.y if y is None else y), (self.c if c is None else c)
        return (self.z, y, 2 * x + c)

    def part(self, x, off, n, k, c=None):
        c = self.c if c is None else c
        row = pl.multiple_of((2 * x + c) * self.block + off, self.block // 4)
        return self.full.at[k, pl.ds(row, n), :]

    def mine(self, off, n, k):
        if self.own is None:
            return self.part(self.x, off, n, k)
        return self.own.at[pl.ds(pl.multiple_of(off, self.block // 4), n), ds(k, self.width)]

    def send(self, src, dst, sem, k, to):
        return pltpu.make_async_remote_copy(src, dst, self.s.at[k], sem.at[k], device_id=to, device_id_type=MESH)

    def first(self, k):
        h = self.block // 2
        o = self.par * h
        return [
            self.send(self.mine(o, h, k), self.part(self.x, o, h, k), self.a, k, self.dev(x=self.p1)),
            self.send(self.mine(o, h, k), self.part(self.x, o, h, k), self.b1, k, self.dev(x=self.p2)),
            self.send(self.mine(0, self.block, k), self.part(self.x, 0, self.block, k), self.e, k, self.dev(c=self.o)),
        ]

    def across(self, x, k):
        q = self.block // 4
        o = self.par * 2 * q
        return [
            self.send(self.part(x, o, q, k), self.part(x, o, q, k), self.ys, k, self.dev(y=(self.y + 1) % 4)),
            self.send(self.part(x, o + q, q, k), self.part(x, o + q, q, k), self.ys, k, self.dev(y=(self.y + 3) % 4)),
        ]

    def over(self, x, half, k):
        h = self.block // 2
        return [self.send(self.part(x, half * h, h, k), self.part(x, half * h, h, k), self.e, k, self.dev(c=self.o))]

    def second(self, k):
        h = self.block // 2
        o = self.par * h
        fwd = [self.send(self.part(self.p1, o, h, k), self.part(self.p1, o, h, k), self.b2, k, self.dev(x=self.p2))]
        return fwd + self.across(self.p1, k) + self.across(self.p2, k) + self.over(self.p1, self.par, k) + self.over(self.p2, self.par, k)

    def third(self, k):
        return self.across(self.opp, k) + self.over(self.opp, self.par, k)

    def fourth(self, k):
        return [d for x in (self.p1, self.p2, self.opp) for d in self.over(x, 1 - self.par, k)]

    def got(self, sem, rows, k):
        r = self.full.at[0, pl.ds(0, rows), :]
        pltpu.make_async_copy(r, r, sem.at[k]).wait()

    def stage(self, i, k):
        h, q = self.block // 2, self.block // 4
        if i == 0:
            sent = self.first(k)
        elif i == 1:
            self.got(self.a, h, k)
            self.got(self.b1, h, k)
            sent = self.second(k)
        elif i == 2:
            self.got(self.b2, h, k)
            sent = self.third(k)
        elif i == 3:
            self.got(self.ys, 6 * q, k)
            sent = self.fourth(k)
        else:
            self.got(self.e, 4 * self.block, k)
            self.got(self.s, 7 * self.block, k)
            return
        for d in sent:
            d.start()


LAGS = (0, 2, 4, 6, 8)


def norm(h):
    wide = h.astype(f32)
    return (wide * lax.rsqrt(jnp.mean(wide * wide, -1, keepdims=True) + 1e-6)).astype(bf16)


dma = pltpu.SemaphoreType.DMA


def turned(to, r, v, size, c):
    t = v.T
    chips = to.shape[0] // size // 2
    for b in range(2 * chips):
        to[ds(chips * ((b + c) % 2) + b // 2, size), r] = t[b * size : (b + 1) * size]


def own_load(w_g, w_u, l, own, sem):
    def one(k):
        for j, w in ((0, w_g), (1, w_u)):
            pltpu.make_async_copy(w.at[l, :, ds(k, C)], own.at[:, ds(2 * k + j, C)], sem).start()
    loop(0, own.shape[1] // (W), one)


def forward_kernel(tm, early, x_h, wg_h, wu_h, wd_h, fgu0, fgu1, fd0, fd1, a0t_h, h1_h, a1_h, a1t_h, act_h, ab_h,
                   xv, av, tv, actv, abv, wv, wdv, own0, own1, ownd, isem, wsem, absem, actsem, own_sem, *gs):
    T, D = x_h.shape
    F = fd0.shape[1]
    n = F // C
    nd = D // C
    where = place()
    z, y, x, c, xs, ys = where
    s = 2 * x + c
    own_load(wg_h, wu_h, 0, own0, own_sem.at[0])
    own_load(wg_h, wu_h, 1, own1, own_sem.at[1])
    xin = pltpu.make_async_copy(x_h, xv, isem.at[0])
    xin.start()
    din = pltpu.make_async_copy(wd_h, ownd, isem.at[1])
    din.start()
    barrier(z, y, x, c, xs)
    for l, own in ((0, own0), (1, own1)):
        pltpu.make_async_copy(own, own, own_sem.at[l]).wait()
    rows, drows = own0.shape[0], wd_h.shape[1]
    kept = ((own0, fgu0), (own1, fgu1), (ownd.at[0], fd0), (ownd.at[1], fd1))

    def keep(i, k):
        own, full = kept[i]
        return pltpu.make_async_copy(own.at[:, ds(k, full.shape[2])], full.at[k, ds(s, own.shape[0]), :], own_sem.at[i])

    g0 = Gather(where, own0, fgu0, rows, W, gs[:6])
    d0 = Gather(where, wd_h.at[0], fd0, drows, C, gs[6:12])
    d1 = Gather(where, wd_h.at[1], fd1, drows, C, gs[12:18])
    g1 = Gather(where, own1, fgu1, rows, W, gs[18:])
    units = ((g0, 0, n), (d0, n, nd), (d1, n + nd, nd), (g1, n + 2 * nd, early))
    total = n + 2 * nd + early

    def tick(t):
        for i, lag in enumerate(LAGS):
            u = t - lag
            for g, base, count in units:
                @pl.when((u >= base) & (u < base + count))
                def _(g=g, i=i, k=u - base):
                    g.stage(i, k)

    lead = LAGS[-1]
    for t in range(2):
        tick(t)
    din.wait()
    for i, (own, full) in enumerate(kept):
        loop(0, full.shape[0], lambda k, i=i: keep(i, k).start())
    xin.wait()

    def start(i):
        r = ds(i, R)
        a = norm(xv[r, :])
        av[r, :] = a
        turned(tv, r, a, rows, c)
    loop(0, T // R, start)
    out0 = pltpu.make_async_copy(tv, a0t_h, isem.at[0])
    out0.start()
    loop(2, lead, lambda t: tick(t))
    for i, (own, full) in enumerate(kept):
        pltpu.make_async_copy(own, own, own_sem.at[i]).wait()

    def wload(k, slot):
        return pltpu.make_async_copy(fgu0.at[k], wv.at[slot], wsem.at[slot])

    def abstore(k, slot):
        return pltpu.make_async_copy(abv.at[slot], ab_h.at[k], absem.at[slot])

    tick(lead)
    wload(0, 0).start()

    def up(k):
        slot = k % 2
        tick(k + 1 + lead)

        @pl.when(k + 1 < n)
        def _():
            wload(k + 1, 1 - slot).start()
        wload(k, slot).wait()

        @pl.when(k >= 2)
        def _():
            abstore(k - 2, slot).wait()

        for i in range(T // tm):
            r = pl.ds(i * tm, tm)
            gu = dot(av[r, :], wv[slot], NN)
            g, u = gu[:, :C], gu[:, C:]
            sg = 0.5 + 0.5 * jnp.tanh(0.5 * g)
            b = g * sg
            actv[r, ds(k, C)] = (b * u).astype(bf16)
            abv[slot, r, :C] = u * (sg + b * (1 - sg))
            abv[slot, r, C:] = b
        abstore(k, slot).start()
        pltpu.make_async_copy(actv.at[:, ds(k, C)], act_h.at[k], actsem).start()
    loop(0, n, up)

    def dload(j, slot):
        return pltpu.make_async_copy(fd0.at[j], wdv.at[slot], wsem.at[2 + slot])

    dload(0, 0).start()
    out0.wait()

    def down(j):
        slot = j % 2
        tick(n + j + 1 + lead)

        @pl.when(j + 1 < nd)
        def _():
            dload(j + 1, 1 - slot).start()
        dload(j, slot).wait()
        for i in range(T // tm):
            r = pl.ds(i * tm, tm)
            av[r, ds(j, C)] = dot(actv[r, :], wdv[slot], NN).astype(bf16)
    loop(0, nd, down)
    for k in (n - 2, n - 1):
        abstore(k, k % 2).wait()
    pltpu.make_async_copy(act_h, act_h, actsem).wait()

    def mid(i):
        r = ds(i, R)
        h = (xv[r, :].astype(f32) + av[r, :].astype(f32)).astype(bf16)
        xv[r, :] = h
        a = norm(h)
        av[r, :] = a
        turned(tv, r, a, rows, c)
    loop(0, T // R, mid)
    outs = [pltpu.make_async_copy(v, h, isem.at[i]) for i, (v, h) in enumerate(((xv, h1_h), (av, a1_h), (tv, a1t_h)))]
    for d in outs:
        d.start()
    loop(n + nd + 1 + lead, total + lead, lambda t: tick(t))
    for d in outs:
        d.wait()


def forward(x, wg, wu, wd, tm, early):
    T, D = x.shape
    F = wg.shape[2]
    rows, drows = wg.shape[1], wd.shape[1]
    n, nd = F // C, D // C
    S = jax.ShapeDtypeStruct
    out = (S((n, D, W), bf16), S((n, D, W), bf16), S((nd, F, C), bf16), S((nd, F, C), bf16), S((D, T), bf16), S((T, D), bf16),
           S((T, D), bf16), S((D, T), bf16), S((n, T, C), bf16), S((n, T, W), f32))
    return pl.pallas_call(
        functools.partial(forward_kernel, tm, early),
        out_shape=out,
        in_specs=[pl.BlockSpec(memory_space=pl.ANY)] * 4,
        out_specs=[pl.BlockSpec(memory_space=pl.ANY)] * len(out),
        scratch_shapes=[
            pltpu.VMEM((T, D), bf16), pltpu.VMEM((T, D), bf16), pltpu.VMEM((D, T), bf16), pltpu.VMEM((T, F), bf16),
            pltpu.VMEM((2, T, W), f32), pltpu.VMEM((2, D, W), bf16), pltpu.VMEM((2, F, C), bf16),
            pltpu.VMEM((rows, 2 * F), bf16), pltpu.VMEM((rows, 2 * F), bf16), pltpu.VMEM((2, drows, D), bf16),
            dma((3,)), dma((4,)), dma((2,)), dma(()), dma((4,)),
        ] + [dma((n,))] * 6 + [dma((nd,))] * 12 + [dma((early,))] * 6,
        compiler_params=pltpu.CompilerParams(collective_id=0, has_side_effects=True, vmem_limit_bytes=62 * 2**20),
        name="forward",
    )(x, wg, wu, wd)
class Scatter:
    def __init__(self, where, sems):
        self.z, self.y, self.x, self.c, (self.p1, self.p2), (self.q1, self.q2) = where
        self.xo, self.yo = (self.x + 2) % 4, (self.y + 2) % 4
        self.o = 1 - self.c
        self.snd, self.rcv = sems

    def put(self, src, dst, i, k, x=None, y=None, c=None):
        x, y, c = (self.x if x is None else x), (self.y if y is None else y), (self.c if c is None else c)
        return pltpu.make_async_remote_copy(src, dst, self.snd.at[i, k], self.rcv.at[i, k], device_id=(self.z, y, 2 * x + c), device_id_type=MESH)

    def stage(self, i, t):
        if i > 0:
            k, r = self.whole(i - 1, t)
            pltpu.make_async_copy(r, r, self.snd.at[i - 1, k]).wait()
            pltpu.make_async_copy(r, r, self.rcv.at[i - 1, k]).wait()
            self.work(i, t)
        for d in self.sent(i, t):
            d.start()

    def tick(self, t, units, mid):
        for i in reversed(range(len(self.due))):
            lag, when = self.due[i]
            if when == mid:
                u = t - lag

                @pl.when((u >= 0) & (u < units))
                def _(i=i, u=u):
                    self.stage(i, u)


def wide(v):
    return v.astype(f32)


class ScatterUp(Scatter):
    due = ((1, 0), (1, 1), (3, 0), (4, 1), (5, 1), (6, 1), (7, 1), (8, 1))

    def __init__(self, where, sems, *refs):
        super().__init__(where, sems)
        self.keep, self.give, self.l0, self.s1, self.l1, self.s2, self.l2, self.s3, self.l3, self.kg, self.s4, self.l4, self.gf = refs
        self.rows, self.q = self.l2.shape[1], self.l4.shape[1]

    def final(self, u, j):
        return self.gf.at[u, ds(j, self.q), :]

    def sent(self, i, u):
        k, h = u % SLOTS, u % 2
        if i == 0:
            return [self.put(self.give, self.l0.at[k], i, k, c=self.o)]
        if i == 1:
            return [self.put(self.s1.at[h], self.l1.at[k], i, k, x=self.p1)]
        if i == 2:
            return [self.put(self.s2.at[h], self.l2.at[k], i, k, x=self.p2)]
        if i == 3:
            return [self.put(self.s3.at[h], self.l3.at[k], i, k, y=self.q1)]
        if i == 4:
            return [self.put(self.s4.at[h], self.l4.at[k], i, k, y=self.q2)]
        if i == 5:
            return [self.put(self.final(u, self.y), self.final(u, self.y), i, k, y=self.q2)]
        if i == 6:
            return [self.put(self.final(u, j), self.final(u, j), i, k, y=self.q1) for j in (self.y, self.q2)]
        return []

    def whole(self, i, u):
        k = u % SLOTS
        refs = (self.l0.at[k], self.l1.at[k], self.l2.at[k], self.l3.at[k], self.l4.at[k], self.gf.at[u, ds(0, self.q), :],
                self.gf.at[u, ds(0, 2 * self.q), :])
        return k, refs[i]

    def pair(self, k, b):
        return wide(self.keep[k, ds(b, self.rows), :]) + wide(self.l0[k, ds(b, self.rows), :])

    def work(self, i, u):
        k, h = u % SLOTS, u % 2
        if i == 1:
            self.s1[h, 0] = self.pair(k, self.p1).astype(bf16)
            self.s1[h, 1] = self.pair(k, self.xo).astype(bf16)
        elif i == 2:
            self.s2[h] = (self.pair(k, self.p2) + wide(self.l1[k, 1])).astype(bf16)
        elif i == 3:
            for j, (to, at) in enumerate(((self.q1, 0), (self.yo, 1), (self.y, 0), (self.q2, 1))):
                r = ds(to, self.q)
                rb = pl.ds(pl.multiple_of(self.x * self.rows + to * self.q, self.q), self.q)
                g = (wide(self.keep[k, rb, :]) + wide(self.l0[k, rb, :])) + (wide(self.l1[k, 0, r, :]) + wide(self.l2[k, r, :]))
                if j < 2:
                    self.s3[h, at] = g.astype(bf16)
                else:
                    self.kg[k, at] = g
        elif i == 4:
            self.s4[h] = (self.kg[k, 1] + wide(self.l3[k, 1])).astype(bf16)
        elif i == 5:
            self.gf[u, ds(self.y, self.q), :] = (self.kg[k, 0] + wide(self.l3[k, 0]) + wide(self.l4[k])).astype(bf16)


class ScatterDown(Scatter):
    due = ((1, 0), (1, 1), (3, 0), (4, 1))

    def __init__(self, where, sems, count, *refs):
        super().__init__(where, sems)
        self.keep, self.give, self.m0, self.t1, self.m1, self.t2, self.m2, self.part = refs
        self.count, self.q = count, self.m2.shape[2]

    def sent(self, i, u):
        k, h = u % SLOTS, u % 2
        if i == 0:
            return [self.put(self.give.at[h], self.m0.at[k], i, k, c=self.o)]
        if i == 1:
            return [self.put(self.t1.at[h], self.m1.at[k], i, k, y=self.q1)]
        if i == 2:
            return [self.put(self.t2.at[h], self.m2.at[k], i, k, y=self.q2)]
        return []

    def whole(self, i, u):
        k = u % SLOTS
        return k, (self.m0.at[k], self.m1.at[k], self.m2.at[k])[i]

    def pair(self, k, j):
        return wide(self.keep[k, :, ds(j, self.q)]) + wide(self.m0[k, :, ds(j, self.q)])

    def work(self, i, u):
        k, h = u % SLOTS, u % 2
        if i == 1:
            self.t1[h, 0] = self.pair(k, self.q1).astype(bf16)
            self.t1[h, 1] = self.pair(k, self.yo).astype(bf16)
        elif i == 2:
            self.t2[h] = (self.pair(k, self.q2) + wide(self.m1[k, 1])).astype(bf16)
        elif i == 3:
            n, late = self.m2.shape[1], u // self.count
            self.part[1 - late, ds(u - late * self.count, n), :] = (self.pair(k, self.y) + (wide(self.m1[k, 0]) + wide(self.m2[k]))).astype(bf16)


class ScatterEnd(Scatter):
    def __init__(self, where, sems, part, n1, u, n2, w, dg):
        super().__init__(where, sems)
        self.part, self.n1, self.u, self.n2, self.w, self.dg = part, n1, u, n2, w, dg
        self.rows = n2.shape[1]

    def sent(self, i, l):
        here, there = 4 * self.c + self.y, 4 * (self.o) + self.y
        dg = self.dg
        if i == 0:
            return [self.put(self.part.at[l, ds(b, self.rows), :], self.n1.at[l, j], 0, l, x=self.p1) for j, b in enumerate((self.p1, self.xo))]
        if i == 1:
            return [self.put(self.u.at[l], self.n2.at[l], 1, l, x=self.p2)]
        if i == 2:
            return [self.put(self.w.at[l], dg.at[l, here], 2, l, c=self.o)]
        if i == 3:
            return [self.put(dg.at[l, j], dg.at[l, j], 3, l, y=self.q2) for j in (here, there)]
        if i == 4:
            js = [here, there, 4 * self.c + self.q2, 4 * (self.o) + self.q2]
            return [self.put(dg.at[l, j], dg.at[l, j], 4, l, y=self.q1) for j in js]
        return []

    def whole(self, i, l):
        refs = (self.n1.at[l], self.n2.at[l], self.w.at[l], self.dg.at[l, pl.ds(0, 2)], self.dg.at[l, pl.ds(0, 4)])
        return l, refs[i]

    def work(self, i, l):
        h = self.rows // 2
        if i == 1:
            self.u[l] = (wide(self.part[l, ds(self.p2, self.rows), :]) + wide(self.n1[l, 1])).astype(bf16)
        elif i == 2:
            for mine, c in ((True, self.c), (False, self.o)):
                r = ds(c, h)
                rp = pl.ds(pl.multiple_of(self.x * self.rows + c * h, h), h)
                v = (wide(self.part[l, rp, :]) + (wide(self.n1[l, 0, r, :]) + wide(self.n2[l, r, :]))).astype(bf16)
                if mine:
                    self.dg[l, 4 * self.c + self.y] = v
                else:
                    self.w[l] = v


SLOTS = 5
AHEAD = 8


def backward_kernel(tm, early, dy_h, _, fd0, fd1, a0t_h, h1_h, a1_h, a1t_h, act_h, ab_h, fgu1, gf_h, dg_h,
                    av, atv, dyv, dytv, acc, wv, wdv, actv, dguv,
                    keep, give, l0, s1, l1, s2, l2, s3, l3, kg, s4, l4, gf, dkeep, dgive, m0, t1, m1, t2, m2, part, n1, eu, n2, ew, dg,
                    isem, wsem, us, ur, dsd, dr, es, er, *gs):
    T, D = dy_h.shape
    n = fgu1.shape[0]
    nd = D // C
    nn = n + n
    half = D // 2
    rows = l2.shape[1]
    where = place()
    z, y, x, c, xs, ys = where
    ins = [pltpu.make_async_copy(a, b, isem.at[i]) for i, (a, b) in enumerate(((a1_h, av), (a1t_h, atv), (dy_h, dyv)))]
    for d in ins:
        d.start()

    def load_up(k, slot):
        return pltpu.make_async_copy(fgu1.at[k], wv.at[slot], wsem.at[0, slot])

    def start_down(fd, k, slot):
        for j in range(nd):
            pltpu.make_async_copy(fd.at[j, ds(k, C), :], wdv.at[slot, :, ds(j, C)], wsem.at[1, slot]).start()

    def wait_down(slot):
        pltpu.make_async_copy(wdv.at[slot], wdv.at[slot], wsem.at[1, slot]).wait()

    load_up(0, 0).start()
    start_down(fd1, 0, 0)
    barrier(z, y, x, c, xs)
    g1 = Gather(where, None, fgu1, rows, W, gs)
    up = ScatterUp(where, (us, ur), keep, give, l0, s1, l1, s2, l2, s3, l3, kg, s4, l4, gf)
    down = ScatterDown(where, (dsd, dr), n, dkeep, dgive, m0, t1, m1, t2, m2, part)
    end = ScatterEnd(where, (es, er), part, n1, eu, n2, ew, dg)

    def gather_tick(t):
        for i in range(5):
            @pl.when((t >= i) & (t < n - early + i))
            def _(i=i):
                g1.stage(i, t - i + early)

    def end_tick(t, l):
        for i in range(6):
            @pl.when(t == 2 * i)
            def _(i=i):
                end.stage(i, l)

    def turn_dy(r, v):
        turned(dytv, r, v, half, c)

    for d in ins:
        d.wait()

    def turn(i):
        r = ds(i, R)
        turn_dy(r, dyv[r, :])
    loop(0, T // R, turn)
    acc[...] = jnp.zeros_like(acc)

    def up_gradient(u):
        g = dot(atv[...], dguv[...], NN).astype(bf16)
        keep[u % SLOTS] = g[:half]
        give[...] = g[half:]

    def down_gradient(act, u):
        g = dot(dytv[...], act, NN).astype(bf16).T
        dkeep[u % SLOTS] = g[:, :half]
        dgive[u % 2] = g[:, half:]

    def layer1(k):
        slot = k % 2
        up.tick(k, nn, 0)
        down.tick(k, nn, 0)
        gather_tick(k)

        @pl.when(k + 1 < n)
        def _():
            load_up(k + 1, 1 - slot).start()
            start_down(fd1, k + 1, 1 - slot)
        load_up(k, slot).wait()
        wait_down(slot)
        for i in range(T // tm):
            r = pl.ds(i * tm, tm)
            gu = dot(av[r, :], wv[slot], NN)
            d = wide(dot(dyv[r, :], wdv[slot], NT).astype(bf16))
            g, u = gu[:, :C], gu[:, C:]
            sg = 0.5 + 0.5 * jnp.tanh(0.5 * g)
            b = g * sg
            actv[0, r, :] = (b * u).astype(bf16)
            dguv[r, :C] = (d * (u * (sg + b * (1 - sg)))).astype(bf16)
            dguv[r, C:] = (d * b).astype(bf16)
        up.tick(k, nn, 1)
        down.tick(k, nn, 1)
        down_gradient(actv[0], k)
        up_gradient(k)
        for j in range(2):
            acc[j] += dot(dguv[...], wv[slot, ds(j, half), :], NT)
    loop(0, n, layer1)

    def load_act(k, slot):
        return pltpu.make_async_copy(act_h.at[k], actv.at[slot], wsem.at[2, slot])

    load_act(0, 0).start()
    h_in = pltpu.make_async_copy(h1_h, av, isem.at[0])
    h_in.start()
    at_in = pltpu.make_async_copy(a0t_h, atv, isem.at[1])
    at_in.start()
    start_down(fd0, 0, 0)
    h_in.wait()

    def between(i):
        r = ds(i, R)
        h = wide(av[r, :])
        scale = lax.rsqrt(jnp.mean(h * h, -1, keepdims=True) + 1e-6)
        da = wide(jnp.concatenate([acc[0, r, :], acc[1, r, :]], axis=1).astype(bf16))
        dh = scale * (da - h * (scale * scale) * jnp.mean(da * h, -1, keepdims=True))
        v = (wide(dyv[r, :]) + wide(dh.astype(bf16))).astype(bf16)
        dyv[r, :] = v
        turn_dy(r, v)
    loop(0, T // R, between)

    def load_ab(k, slot):
        return pltpu.make_async_copy(ab_h.at[k], acc.at[slot], wsem.at[3, slot])

    load_ab(0, 0).start()

    def layer0_down(k):
        slot = k % 2
        down.tick(n + k, nn, 0)

        @pl.when(k + 1 < n)
        def _():
            load_act(k + 1, 1 - slot).start()
        load_act(k, slot).wait()

    def ahead(k):
        layer0_down(k)
        end_tick(k - 4, 1)
        down_gradient(actv[k % 2], n + k)
        down.tick(n + k, nn, 1)
    loop(0, AHEAD, ahead)
    at_in.wait()

    def layer0(k, both):
        slot = k % 2
        up.tick(n + k, nn, 0)

        @pl.when(k + 1 < n)
        def _():
            load_ab(k + 1, 1 - slot).start()
            start_down(fd0, k + 1, 1 - slot)
        if both:
            layer0_down(k + AHEAD)
        else:
            down.tick(n + AHEAD + k, nn, 0)
        end_tick(k + AHEAD - 4, 1)
        end_tick(k - (n - AHEAD + 4), 0)
        load_ab(k, slot).wait()
        wait_down(slot)
        for i in range(T // tm):
            r = pl.ds(i * tm, tm)
            d = wide(dot(dyv[r, :], wdv[slot], NT).astype(bf16))
            dguv[r, :C] = (d * acc[slot, r, :C]).astype(bf16)
            dguv[r, C:] = (d * acc[slot, r, C:]).astype(bf16)
        if both:
            down_gradient(actv[(k + AHEAD) % 2], n + AHEAD + k)
        up.tick(n + k, nn, 1)
        down.tick(n + AHEAD + k, nn, 1)
        up_gradient(n + k)
    loop(0, n - AHEAD, lambda k: layer0(k, True))
    loop(n - AHEAD, n, lambda k: layer0(k, False))

    def rest(t):
        up.tick(n + t, nn, 0)
        end_tick(t - (n - AHEAD + 4), 0)
        up.tick(n + t, nn, 1)
    loop(n, n + up.due[-1][0], rest)
    outs = [pltpu.make_async_copy(gf, gf_h, isem.at[0]), pltpu.make_async_copy(dg, dg_h, isem.at[1])]
    for d in outs:
        d.start()
    for d in outs:
        d.wait()


def backward(dy, fgu1, fd0, fd1, a0t, h1, a1, a1t, act, ab, tm, early):
    T, D = dy.shape
    n = fgu1.shape[0]
    F = n * C
    rows, drows = D // 8, F // 8
    nn = n + n
    S = jax.ShapeDtypeStruct
    out = (S(fgu1.shape, bf16), S((nn, rows, W), bf16), S((2, 8, drows, rows), bf16))
    q, w = rows // 4, W

    def V(*shape, dtype=bf16):
        return pltpu.VMEM(shape, dtype)
    return pl.pallas_call(
        functools.partial(backward_kernel, tm, early),
        out_shape=out,
        in_specs=[pl.BlockSpec(memory_space=pl.ANY)] * 10,
        out_specs=[pl.BlockSpec(memory_space=pl.ANY)] * 3,
        input_output_aliases={1: 0},
        scratch_shapes=[
            V(T, D), V(D, T), V(T, D), V(D, T), V(2, T, w, dtype=f32), V(2, D, w), V(2, C, D), V(2, T, C), V(T, w),
            V(SLOTS, D // 2, w), V(D // 2, w), V(SLOTS, D // 2, w), V(2, 2, rows, w), V(SLOTS, 2, rows, w), V(2, rows, w), V(SLOTS, rows, w),
            V(2, 2, q, w), V(SLOTS, 2, q, w), V(SLOTS, 2, q, w, dtype=f32), V(2, q, w), V(SLOTS, q, w), V(nn, rows, w),
            V(SLOTS, C, D // 2), V(2, C, D // 2), V(SLOTS, C, D // 2), V(2, 2, C, rows), V(SLOTS, 2, C, rows), V(2, C, rows), V(SLOTS, C, rows),
            V(2, F, rows), V(2, 2, 2 * drows, rows), V(2, 2 * drows, rows), V(2, 2 * drows, rows), V(2, drows, rows), V(2, 8, drows, rows),
            dma((3,)), dma((4, 2)), dma((7, SLOTS)), dma((7, SLOTS)), dma((3, SLOTS)), dma((3, SLOTS)), dma((5, 2)), dma((5, 2)),
        ] + [dma((n,))] * 6,
        compiler_params=pltpu.CompilerParams(collective_id=1, has_side_effects=True, vmem_limit_bytes=63 * 2**20),
        name="backward",
    )(dy, fgu1, fd0, fd1, a0t, h1, a1, a1t, act, ab)


def adamw(w, m, v, g):
    m = 0.9 * m + 0.1 * g
    v = 0.95 * v + 0.05 * g * g
    step = m * lax.rsqrt(v + 1e-8) + 0.1 * w
    return (w - 0.02 * step).astype(bf16), m, v


def update_kernel(gf, dg, wg, wu, wd, mg, mu, md, vg, vu, vd, *outs):
    def one(part, at, w, m, v, g):
        for o, val in zip(outs[part::3], adamw(wide(w[at]), m[at], v[at], wide(g)), strict=True):
            o[at] = val

    n, _, w = gf.shape
    for k in range(n):
        at = (0, slice(None), pl.ds(k * C, C))
        one(0, at, wg, mg, vg, gf[k, :, :C])
        one(1, at, wu, mu, vu, gf[k, :, C:])
    w = dg.shape[3]
    for j in range(dg.shape[1]):
        one(2, (0, slice(None), pl.ds(j * w, w)), wd, md, vd, dg[0, j])


def update(gf, dg, *arrays):
    wg, wd = arrays[0], arrays[2]
    n = wg.shape[2] // C
    S = jax.ShapeDtypeStruct
    up = pl.BlockSpec((1, wg.shape[1] // PARTS, wg.shape[2]), lambda l, k: (l, k, 0))
    down = pl.BlockSpec((1, wd.shape[1] // PARTS, wd.shape[2]), lambda l, k: (l, k, 0))
    specs = [up, up, down] * 3
    gspec = [pl.BlockSpec((n, gf.shape[1] // PARTS, gf.shape[2]), lambda l, k: (1 - l, k, 0)),
             pl.BlockSpec((1, dg.shape[1], dg.shape[2] // PARTS, dg.shape[3]), lambda l, k: (l, 0, k, 0))]
    return pl.pallas_call(
        update_kernel,
        grid=(2, PARTS),
        out_shape=tuple(S(a.shape, a.dtype) for a in arrays),
        in_specs=gspec + specs,
        out_specs=specs,
        name="update",
    )(gf, dg, *arrays)


PARTS = 4
TM, EARLY = 512, 5


def solution(mesh):
    assert mesh.shape["r"] == 4 and mesh.shape["s"] == 8

    def step(x, dy, *arrays):
        _, fgu1, fd0, fd1, a0t, h1, a1, a1t, act, ab = forward(x[0], *arrays[:3], TM, EARLY)
        _, gf, dg = backward(dy[0], fgu1, fd0, fd1, a0t, h1, a1, a1t, act, ab, TM, EARLY)
        return update(gf, dg, *arrays)

    states, cut = P(("rep", "r", "s"), None, None), P(None, "s", None)
    return jax.shard_map(
        step,
        mesh=mesh,
        in_specs=(states, states) + (cut,) * 9,
        out_specs=(P("rep", "s", None),) * 9,
        check_vma=False,
    )
```

```python
import functools
import jax
import jax.numpy as jnp
from jax import lax
from jax.experimental import pallas as pl
from jax.experimental.pallas import tpu as pltpu
from jax.sharding import PartitionSpec as P

bf16, f32 = jnp.bfloat16, jnp.float32
C = 256
W = C + C
R = 256
MESH = pl.DeviceIdType.MESH
NN, NT = ((1,), (0,)), ((1,), (1,))


def dot(a, b, dims):
    return lax.dot_general(a, b, (dims, ((), ())), preferred_element_type=f32)


def ds(i, n):
    return pl.ds(pl.multiple_of(i * n, n), n)


def loop(last, f, first=0):
    def body(i, _):
        f(i)
        return 0
    lax.fori_loop(first, last, body, 0)


def place():
    z, y, s = (lax.axis_index(n) for n in ("rep", "r", "s"))
    x, c = s // 2, s % 2

    def pair(i):
        near, far = i + 1 - 2 * (i % 2), 3 - i
        return (1 - c) * near + c * far, c * near + (1 - c) * far

    return z, y, x, c, pair(x), pair(y)


def barrier(z, y, x, c, xs):
    sem = pltpu.get_barrier_semaphore()
    others = [(z, y, 2 * x + 1 - c)] + [(z, y, 2 * p + c) for p in xs] + [(z, (y + d) % 4, 2 * x + c) for d in (1, 3)]
    for o in others:
        pl.semaphore_signal(sem, inc=1, device_id=o, device_id_type=MESH)
    pl.semaphore_wait(sem, len(others))
    return others


class Gather:
    def __init__(self, where, own, full, block, width, sems):
        self.z, self.y, self.x, self.c, (self.p1, self.p2), _ = where
        self.own, self.full, self.block, self.width = own, full, block, width
        self.a, self.b1, self.b2, self.ys, self.e, self.s = sems
        self.opp = (self.x + 2) % 4
        self.o = 1 - self.c
        self.par = self.y % 2

    def dev(self, x=None, y=None, c=None):
        x, y, c = (self.x if x is None else x), (self.y if y is None else y), (self.c if c is None else c)
        return (self.z, y, 2 * x + c)

    def part(self, x, off, n, k, c=None):
        c = self.c if c is None else c
        row = pl.multiple_of((2 * x + c) * self.block + off, self.block // 4)
        return self.full.at[k, pl.ds(row, n), :]

    def mine(self, off, n, k):
        if self.own is None:
            return self.part(self.x, off, n, k)
        return self.own.at[pl.ds(pl.multiple_of(off, self.block // 4), n), ds(k, self.width)]

    def send(self, src, dst, sem, k, to):
        return pltpu.make_async_remote_copy(src, dst, self.s.at[k], sem.at[k], device_id=to, device_id_type=MESH)

    def first(self, k):
        h = self.block // 2
        o = self.par * h
        return [
            self.send(self.mine(o, h, k), self.part(self.x, o, h, k), self.a, k, self.dev(x=self.p1)),
            self.send(self.mine(o, h, k), self.part(self.x, o, h, k), self.b1, k, self.dev(x=self.p2)),
            self.send(self.mine(0, self.block, k), self.part(self.x, 0, self.block, k), self.e, k, self.dev(c=self.o)),
        ]

    def across(self, x, k):
        q = self.block // 4
        o = self.par * 2 * q
        return [
            self.send(self.part(x, o, q, k), self.part(x, o, q, k), self.ys, k, self.dev(y=(self.y + 1) % 4)),
            self.send(self.part(x, o + q, q, k), self.part(x, o + q, q, k), self.ys, k, self.dev(y=(self.y + 3) % 4)),
        ]

    def over(self, x, half, k):
        h = self.block // 2
        return [self.send(self.part(x, half * h, h, k), self.part(x, half * h, h, k), self.e, k, self.dev(c=self.o))]

    def second(self, k):
        h = self.block // 2
        o = self.par * h
        fwd = [self.send(self.part(self.p1, o, h, k), self.part(self.p1, o, h, k), self.b2, k, self.dev(x=self.p2))]
        return fwd + self.across(self.p1, k) + self.across(self.p2, k) + self.over(self.p1, self.par, k) + self.over(self.p2, self.par, k)

    def third(self, k):
        return self.across(self.opp, k) + self.over(self.opp, self.par, k)

    def fourth(self, k):
        return [d for x in (self.p1, self.p2, self.opp) for d in self.over(x, 1 - self.par, k)]

    def got(self, sem, rows, k):
        r = self.full.at[0, pl.ds(0, rows), :]
        pltpu.make_async_copy(r, r, sem.at[k]).wait()

    def stage(self, i, k):
        h, q = self.block // 2, self.block // 4
        if i == 0:
            sent = self.first(k)
        elif i == 1:
            self.got(self.a, h, k)
            self.got(self.b1, h, k)
            sent = self.second(k)
        elif i == 2:
            self.got(self.b2, h, k)
            sent = self.third(k)
        elif i == 3:
            self.got(self.ys, 6 * q, k)
            sent = self.fourth(k)
        else:
            self.got(self.e, 4 * self.block, k)
            self.got(self.s, 7 * self.block, k)
            return
        for d in sent:
            d.start()


LAGS = (0, 2, 4, 6, 8)


def norm(h):
    wide = h.astype(f32)
    return (wide * lax.rsqrt(jnp.mean(wide * wide, -1, keepdims=True) + 1e-6)).astype(bf16)


dma = pltpu.SemaphoreType.DMA


def turned(to, r, v, size, c):
    t = v.T
    chips = to.shape[0] // size // 2
    for b in range(2 * chips):
        to[ds(chips * ((b + c) % 2) + b // 2, size), r] = t[b * size : (b + 1) * size]


def own_load(w_g, w_u, l, own, sem):
    def one(k):
        for j, w in ((0, w_g), (1, w_u)):
            pltpu.make_async_copy(w.at[l, :, ds(k, C)], own.at[:, ds(2 * k + j, C)], sem).start()
    loop(own.shape[1] // (W), one)


def forward_kernel(tm, early, x_h, wg_h, wu_h, wd_h, fgu0, fgu1, fd0, fd1, a0t_h, h1_h, a1_h, a1t_h, act_h, ab_h,
                   xv, av, tv, actv, abv, wv, wdv, own0, own1, ownd, isem, wsem, absem, actsem, own_sem, *gs):
    T, D = x_h.shape
    F = fd0.shape[1]
    n = F // C
    nd = D // C
    where = place()
    z, y, x, c, xs, ys = where
    s = 2 * x + c
    own_load(wg_h, wu_h, 0, own0, own_sem.at[0])
    own_load(wg_h, wu_h, 1, own1, own_sem.at[1])
    xin = pltpu.make_async_copy(x_h, xv, isem.at[0])
    xin.start()
    din = pltpu.make_async_copy(wd_h, ownd, isem.at[1])
    din.start()
    barrier(z, y, x, c, xs)
    for l, own in ((0, own0), (1, own1)):
        pltpu.make_async_copy(own, own, own_sem.at[l]).wait()
    rows, drows = own0.shape[0], wd_h.shape[1]
    kept = ((own0, fgu0), (own1, fgu1), (ownd.at[0], fd0), (ownd.at[1], fd1))

    def keep(i, k):
        own, full = kept[i]
        return pltpu.make_async_copy(own.at[:, ds(k, full.shape[2])], full.at[k, ds(s, own.shape[0]), :], own_sem.at[i])

    g0 = Gather(where, own0, fgu0, rows, W, gs[:6])
    d0 = Gather(where, wd_h.at[0], fd0, drows, C, gs[6:12])
    d1 = Gather(where, wd_h.at[1], fd1, drows, C, gs[12:18])
    g1 = Gather(where, own1, fgu1, rows, W, gs[18:])
    units = ((g0, 0, n), (d0, n, nd), (d1, n + nd, nd), (g1, n + 2 * nd, early))
    total = n + 2 * nd + early

    def tick(t, lo=None, hi=None):
        lo, hi = (t, t) if lo is None else (lo, hi)
        for i, lag in enumerate(LAGS):
            for g, base, count in units:
                first, last = base + lag, base + lag + count - 1
                if hi < first or lo > last:
                    continue
                if lo >= first and hi <= last:
                    g.stage(i, t - first)
                    continue

                @pl.when((t >= first) & (t <= last))
                def _(g=g, i=i, k=t - first):
                    g.stage(i, k)

    lead = LAGS[-1]
    for t in range(2):
        tick(t)
    din.wait()
    for i, (own, full) in enumerate(kept):
        loop(full.shape[0], lambda k, i=i: keep(i, k).start())
    xin.wait()

    def start(i):
        r = ds(i, R)
        a = norm(xv[r, :])
        av[r, :] = a
        turned(tv, r, a, rows, c)
    loop(T // R, start)
    out0 = pltpu.make_async_copy(tv, a0t_h, isem.at[0])
    out0.start()
    loop(lead, lambda t: tick(t, 2, lead - 1), 2)
    for i, (own, full) in enumerate(kept):
        pltpu.make_async_copy(own, own, own_sem.at[i]).wait()

    def wload(k, slot):
        return pltpu.make_async_copy(fgu0.at[k], wv.at[slot], wsem.at[slot])

    def abstore(k, slot):
        return pltpu.make_async_copy(abv.at[slot], ab_h.at[k], absem.at[slot])

    tick(lead)
    wload(0, 0).start()

    def up(k):
        slot = k % 2
        tick(k + 1 + lead, 1 + lead, n + lead)

        @pl.when(k + 1 < n)
        def _():
            wload(k + 1, 1 - slot).start()
        wload(k, slot).wait()

        @pl.when(k >= 2)
        def _():
            abstore(k - 2, slot).wait()

        for i in range(T // tm):
            r = pl.ds(i * tm, tm)
            gu = dot(av[r, :], wv[slot], NN)
            g, u = gu[:, :C], gu[:, C:]
            sg = 0.5 + 0.5 * jnp.tanh(0.5 * g)
            b = g * sg
            actv[r, ds(k, C)] = (b * u).astype(bf16)
            abv[slot, r, :C] = u * (sg + b * (1 - sg))
            abv[slot, r, C:] = b
        abstore(k, slot).start()
        pltpu.make_async_copy(actv.at[:, ds(k, C)], act_h.at[k], actsem).start()
    loop(n, up)

    def dload(j, slot):
        return pltpu.make_async_copy(fd0.at[j], wdv.at[slot], wsem.at[2 + slot])

    dload(0, 0).start()
    out0.wait()

    def down(j):
        slot = j % 2
        tick(n + j + 1 + lead, n + 1 + lead, n + nd + lead)

        @pl.when(j + 1 < nd)
        def _():
            dload(j + 1, 1 - slot).start()
        dload(j, slot).wait()
        for i in range(T // tm):
            r = pl.ds(i * tm, tm)
            av[r, ds(j, C)] = dot(actv[r, :], wdv[slot], NN).astype(bf16)
    loop(nd, down)
    for k in (n - 2, n - 1):
        abstore(k, k % 2).wait()
    pltpu.make_async_copy(act_h, act_h, actsem).wait()

    def mid(i):
        r = ds(i, R)
        h = (xv[r, :].astype(f32) + av[r, :].astype(f32)).astype(bf16)
        xv[r, :] = h
        a = norm(h)
        av[r, :] = a
        turned(tv, r, a, rows, c)
    loop(T // R, mid)
    outs = [pltpu.make_async_copy(v, h, isem.at[i]) for i, (v, h) in enumerate(((xv, h1_h), (av, a1_h), (tv, a1t_h)))]
    for d in outs:
        d.start()
    loop(total + lead, lambda t: tick(t, n + nd + 1 + lead, total + lead - 1), n + nd + 1 + lead)
    for d in outs:
        d.wait()


def forward(x, wg, wu, wd, tm, early):
    T, D = x.shape
    F = wg.shape[2]
    rows, drows = wg.shape[1], wd.shape[1]
    n, nd = F // C, D // C
    S = jax.ShapeDtypeStruct
    out = (S((n, D, W), bf16), S((n, D, W), bf16), S((nd, F, C), bf16), S((nd, F, C), bf16), S((D, T), bf16), S((T, D), bf16),
           S((T, D), bf16), S((D, T), bf16), S((n, T, C), bf16), S((n, T, W), f32))
    return pl.pallas_call(
        functools.partial(forward_kernel, tm, early),
        out_shape=out,
        in_specs=[pl.BlockSpec(memory_space=pl.ANY)] * 4,
        out_specs=[pl.BlockSpec(memory_space=pl.ANY)] * len(out),
        scratch_shapes=[
            pltpu.VMEM((T, D), bf16), pltpu.VMEM((T, D), bf16), pltpu.VMEM((D, T), bf16), pltpu.VMEM((T, F), bf16),
            pltpu.VMEM((2, T, W), f32), pltpu.VMEM((2, D, W), bf16), pltpu.VMEM((2, F, C), bf16),
            pltpu.VMEM((rows, 2 * F), bf16), pltpu.VMEM((rows, 2 * F), bf16), pltpu.VMEM((2, drows, D), bf16),
            dma((3,)), dma((4,)), dma((2,)), dma(()), dma((4,)),
        ] + [dma((n,))] * 6 + [dma((nd,))] * 12 + [dma((early,))] * 6,
        compiler_params=pltpu.CompilerParams(collective_id=0, has_side_effects=True, vmem_limit_bytes=62 * 2**20),
        name="forward",
    )(x, wg, wu, wd)
class Scatter:
    def __init__(self, where, sems):
        self.z, self.y, self.x, self.c, (self.p1, self.p2), (self.q1, self.q2) = where
        self.xo, self.yo = (self.x + 2) % 4, (self.y + 2) % 4
        self.o = 1 - self.c
        self.snd, self.rcv = sems

    def put(self, src, dst, i, k, x=None, y=None, c=None):
        x, y, c = (self.x if x is None else x), (self.y if y is None else y), (self.c if c is None else c)
        return pltpu.make_async_remote_copy(src, dst, self.snd.at[i, k], self.rcv.at[i, k], device_id=(self.z, y, 2 * x + c), device_id_type=MESH)

    def stage(self, i, t):
        if i > 0:
            k, r = self.whole(i - 1, t)
            pltpu.make_async_copy(r, r, self.snd.at[i - 1, k]).wait()
            pltpu.make_async_copy(r, r, self.rcv.at[i - 1, k]).wait()
            self.work(i, t)
        for d in self.sent(i, t):
            d.start()

    def tick(self, t, units, mid):
        for i in reversed(range(len(self.due))):
            lag, when = self.due[i]
            if when == mid:
                u = t - lag

                @pl.when((u >= 0) & (u < units))
                def _(i=i, u=u):
                    self.stage(i, u)


def wide(v):
    return v.astype(f32)


class ScatterUp(Scatter):
    due = ((1, 0), (1, 1), (3, 0), (4, 1), (5, 1), (6, 1), (7, 1), (8, 1))

    def __init__(self, where, sems, *refs):
        super().__init__(where, sems)
        self.keep, self.give, self.l0, self.s1, self.l1, self.s2, self.l2, self.s3, self.l3, self.kg, self.s4, self.l4, self.gf = refs
        self.rows, self.q = self.l2.shape[1], self.l4.shape[1]

    def final(self, u, j):
        return self.gf.at[u, ds(j, self.q), :]

    def sent(self, i, u):
        k, h = u % SLOTS, u % 2
        if i == 0:
            return [self.put(self.give, self.l0.at[k], i, k, c=self.o)]
        if i == 1:
            return [self.put(self.s1.at[h], self.l1.at[k], i, k, x=self.p1)]
        if i == 2:
            return [self.put(self.s2.at[h], self.l2.at[k], i, k, x=self.p2)]
        if i == 3:
            return [self.put(self.s3.at[h], self.l3.at[k], i, k, y=self.q1)]
        if i == 4:
            return [self.put(self.s4.at[h], self.l4.at[k], i, k, y=self.q2)]
        if i == 5:
            return [self.put(self.final(u, self.y), self.final(u, self.y), i, k, y=self.q2)]
        if i == 6:
            return [self.put(self.final(u, j), self.final(u, j), i, k, y=self.q1) for j in (self.y, self.q2)]
        return []

    def whole(self, i, u):
        k = u % SLOTS
        refs = (self.l0.at[k], self.l1.at[k], self.l2.at[k], self.l3.at[k], self.l4.at[k], self.gf.at[u, ds(0, self.q), :],
                self.gf.at[u, ds(0, 2 * self.q), :])
        return k, refs[i]

    def pair(self, k, b):
        return wide(self.keep[k, ds(b, self.rows), :]) + wide(self.l0[k, ds(b, self.rows), :])

    def work(self, i, u):
        k, h = u % SLOTS, u % 2
        if i == 1:
            self.s1[h, 0] = self.pair(k, self.p1).astype(bf16)
            self.s1[h, 1] = self.pair(k, self.xo).astype(bf16)
        elif i == 2:
            self.s2[h] = (self.pair(k, self.p2) + wide(self.l1[k, 1])).astype(bf16)
        elif i == 3:
            for j, (to, at) in enumerate(((self.q1, 0), (self.yo, 1), (self.y, 0), (self.q2, 1))):
                r = ds(to, self.q)
                rb = pl.ds(pl.multiple_of(self.x * self.rows + to * self.q, self.q), self.q)
                g = (wide(self.keep[k, rb, :]) + wide(self.l0[k, rb, :])) + (wide(self.l1[k, 0, r, :]) + wide(self.l2[k, r, :]))
                if j < 2:
                    self.s3[h, at] = g.astype(bf16)
                else:
                    self.kg[k, at] = g
        elif i == 4:
            self.s4[h] = (self.kg[k, 1] + wide(self.l3[k, 1])).astype(bf16)
        elif i == 5:
            self.gf[u, ds(self.y, self.q), :] = (self.kg[k, 0] + wide(self.l3[k, 0]) + wide(self.l4[k])).astype(bf16)


class ScatterDown(Scatter):
    due = ((1, 0), (1, 1), (3, 0), (4, 1))

    def __init__(self, where, sems, count, *refs):
        super().__init__(where, sems)
        self.keep, self.give, self.m0, self.t1, self.m1, self.t2, self.m2, self.part = refs
        self.count, self.q = count, self.m2.shape[2]

    def sent(self, i, u):
        k, h = u % SLOTS, u % 2
        if i == 0:
            return [self.put(self.give.at[h], self.m0.at[k], i, k, c=self.o)]
        if i == 1:
            return [self.put(self.t1.at[h], self.m1.at[k], i, k, y=self.q1)]
        if i == 2:
            return [self.put(self.t2.at[h], self.m2.at[k], i, k, y=self.q2)]
        return []

    def whole(self, i, u):
        k = u % SLOTS
        return k, (self.m0.at[k], self.m1.at[k], self.m2.at[k])[i]

    def pair(self, k, j):
        return wide(self.keep[k, :, ds(j, self.q)]) + wide(self.m0[k, :, ds(j, self.q)])

    def work(self, i, u):
        k, h = u % SLOTS, u % 2
        if i == 1:
            self.t1[h, 0] = self.pair(k, self.q1).astype(bf16)
            self.t1[h, 1] = self.pair(k, self.yo).astype(bf16)
        elif i == 2:
            self.t2[h] = (self.pair(k, self.q2) + wide(self.m1[k, 1])).astype(bf16)
        elif i == 3:
            n, late = self.m2.shape[1], u // self.count
            self.part[1 - late, ds(u - late * self.count, n), :] = (self.pair(k, self.y) + (wide(self.m1[k, 0]) + wide(self.m2[k]))).astype(bf16)


class ScatterEnd(Scatter):
    def __init__(self, where, sems, part, n1, u, n2, w, dg):
        super().__init__(where, sems)
        self.part, self.n1, self.u, self.n2, self.w, self.dg = part, n1, u, n2, w, dg
        self.rows = n2.shape[1]

    def sent(self, i, l):
        here, there = 4 * self.c + self.y, 4 * (self.o) + self.y
        dg = self.dg
        if i == 0:
            return [self.put(self.part.at[l, ds(b, self.rows), :], self.n1.at[l, j], 0, l, x=self.p1) for j, b in enumerate((self.p1, self.xo))]
        if i == 1:
            return [self.put(self.u.at[l], self.n2.at[l], 1, l, x=self.p2)]
        if i == 2:
            return [self.put(self.w.at[l], dg.at[l, here], 2, l, c=self.o)]
        if i == 3:
            return [self.put(dg.at[l, j], dg.at[l, j], 3, l, y=self.q2) for j in (here, there)]
        if i == 4:
            js = [here, there, 4 * self.c + self.q2, 4 * (self.o) + self.q2]
            return [self.put(dg.at[l, j], dg.at[l, j], 4, l, y=self.q1) for j in js]
        return []

    def whole(self, i, l):
        refs = (self.n1.at[l], self.n2.at[l], self.w.at[l], self.dg.at[l, pl.ds(0, 2)], self.dg.at[l, pl.ds(0, 4)])
        return l, refs[i]

    def work(self, i, l):
        h = self.rows // 2
        if i == 1:
            self.u[l] = (wide(self.part[l, ds(self.p2, self.rows), :]) + wide(self.n1[l, 1])).astype(bf16)
        elif i == 2:
            for mine, c in ((True, self.c), (False, self.o)):
                r = ds(c, h)
                rp = pl.ds(pl.multiple_of(self.x * self.rows + c * h, h), h)
                v = (wide(self.part[l, rp, :]) + (wide(self.n1[l, 0, r, :]) + wide(self.n2[l, r, :]))).astype(bf16)
                if mine:
                    self.dg[l, 4 * self.c + self.y] = v
                else:
                    self.w[l] = v


SLOTS = 5
AHEAD = 7


def backward_kernel(tm, early, dy_h, _, fd0, fd1, a0t_h, h1_h, a1_h, a1t_h, act_h, ab_h, fgu1, gf_h, dg_h,
                    av, atv, dyv, dytv, acc, wv, wdv, actv, dguv,
                    keep, give, l0, s1, l1, s2, l2, s3, l3, kg, s4, l4, gf, dkeep, dgive, m0, t1, m1, t2, m2, part, n1, eu, n2, ew, dg,
                    isem, wsem, us, ur, dsd, dr, es, er, *gs):
    T, D = dy_h.shape
    n = fgu1.shape[0]
    nd = D // C
    nn = n + n
    half = D // 2
    rows = l2.shape[1]
    where = place()
    z, y, x, c, xs, ys = where
    ins = [pltpu.make_async_copy(a, b, isem.at[i]) for i, (a, b) in enumerate(((dy_h, dyv), (a1_h, av), (a1t_h, atv)))]
    for d in ins:
        d.start()

    def load_up(k, slot):
        return pltpu.make_async_copy(fgu1.at[k], wv.at[slot], wsem.at[0, slot])

    def start_down(fd, k, slot):
        for j in range(nd):
            pltpu.make_async_copy(fd.at[j, ds(k, C), :], wdv.at[slot, :, ds(j, C)], wsem.at[1, slot]).start()

    def wait_down(slot):
        pltpu.make_async_copy(wdv.at[slot], wdv.at[slot], wsem.at[1, slot]).wait()

    load_up(0, 0).start()
    start_down(fd1, 0, 0)
    barrier(z, y, x, c, xs)
    g1 = Gather(where, None, fgu1, rows, W, gs)
    up = ScatterUp(where, (us, ur), keep, give, l0, s1, l1, s2, l2, s3, l3, kg, s4, l4, gf)
    down = ScatterDown(where, (dsd, dr), n, dkeep, dgive, m0, t1, m1, t2, m2, part)
    end = ScatterEnd(where, (es, er), part, n1, eu, n2, ew, dg)

    def gather_tick(t):
        for i in range(5):
            @pl.when((t >= i) & (t < n - early + i))
            def _(i=i):
                g1.stage(i, t - i + early)

    def end_tick(t, l):
        for i in range(6):
            @pl.when(t == 2 * i)
            def _(i=i):
                end.stage(i, l)

    def turn_dy(r, v):
        turned(dytv, r, v, half, c)

    acc[...] = jnp.zeros_like(acc)
    ins[0].wait()

    def turn(i):
        r = ds(i, R)
        turn_dy(r, dyv[r, :])
    loop(T // R, turn)
    for d in ins[1:]:
        d.wait()

    def up_gradient(u):
        g = dot(atv[...], dguv[...], NN).astype(bf16)
        keep[u % SLOTS] = g[:half]
        give[...] = g[half:]

    def down_gradient(act, u):
        g = dot(dytv[...], act, NN).astype(bf16).T
        dkeep[u % SLOTS] = g[:, :half]
        dgive[u % 2] = g[:, half:]

    def layer1(k):
        slot = k % 2
        up.tick(k, nn, 0)
        down.tick(k, nn, 0)
        gather_tick(k)

        @pl.when(k + 1 < n)
        def _():
            load_up(k + 1, 1 - slot).start()
            start_down(fd1, k + 1, 1 - slot)
        load_up(k, slot).wait()
        wait_down(slot)
        for i in range(T // tm):
            r = pl.ds(i * tm, tm)
            gu = dot(av[r, :], wv[slot], NN)
            d = wide(dot(dyv[r, :], wdv[slot], NT).astype(bf16))
            g, u = gu[:, :C], gu[:, C:]
            sg = 0.5 + 0.5 * jnp.tanh(0.5 * g)
            b = g * sg
            actv[0, r, :] = (b * u).astype(bf16)
            dguv[r, :C] = (d * (u * (sg + b * (1 - sg)))).astype(bf16)
            dguv[r, C:] = (d * b).astype(bf16)
        up.tick(k, nn, 1)
        down.tick(k, nn, 1)
        down_gradient(actv[0], k)
        up_gradient(k)
        for j in range(2):
            acc[j] += dot(dguv[...], wv[slot, ds(j, half), :], NT)
    loop(n, layer1)

    def load_act(k, slot):
        return pltpu.make_async_copy(act_h.at[k], actv.at[slot], wsem.at[2, slot])

    load_act(0, 0).start()
    h_in = pltpu.make_async_copy(h1_h, av, isem.at[0])
    h_in.start()
    at_in = pltpu.make_async_copy(a0t_h, atv, isem.at[1])
    at_in.start()
    start_down(fd0, 0, 0)
    h_in.wait()

    def between(i):
        r = ds(i, R)
        h = wide(av[r, :])
        scale = lax.rsqrt(jnp.mean(h * h, -1, keepdims=True) + 1e-6)
        da = wide(jnp.concatenate([acc[0, r, :], acc[1, r, :]], axis=1).astype(bf16))
        dh = scale * (da - h * (scale * scale) * jnp.mean(da * h, -1, keepdims=True))
        v = (wide(dyv[r, :]) + wide(dh.astype(bf16))).astype(bf16)
        dyv[r, :] = v
        turn_dy(r, v)
    loop(T // R, between)

    def load_ab(k, slot):
        return pltpu.make_async_copy(ab_h.at[k], acc.at[slot], wsem.at[3, slot])

    load_ab(0, 0).start()

    def layer0_down(k):
        slot = k % 2
        down.tick(n + k, nn, 0)

        @pl.when(k + 1 < n)
        def _():
            load_act(k + 1, 1 - slot).start()
        load_act(k, slot).wait()

    def ahead(k):
        layer0_down(k)
        end_tick(k - 4, 1)
        down_gradient(actv[k % 2], n + k)
        down.tick(n + k, nn, 1)
    loop(AHEAD, ahead)
    at_in.wait()

    def layer0(k, both):
        slot = k % 2
        up.tick(n + k, nn, 0)

        @pl.when(k + 1 < n)
        def _():
            load_ab(k + 1, 1 - slot).start()
            start_down(fd0, k + 1, 1 - slot)
        if both:
            layer0_down(k + AHEAD)
        else:
            down.tick(n + AHEAD + k, nn, 0)
        end_tick(k + AHEAD - 4, 1)
        end_tick(k - (n - AHEAD + 4), 0)
        load_ab(k, slot).wait()
        wait_down(slot)
        for i in range(T // tm):
            r = pl.ds(i * tm, tm)
            d = wide(dot(dyv[r, :], wdv[slot], NT).astype(bf16))
            dguv[r, :C] = (d * acc[slot, r, :C]).astype(bf16)
            dguv[r, C:] = (d * acc[slot, r, C:]).astype(bf16)
        if both:
            down_gradient(actv[(k + AHEAD) % 2], n + AHEAD + k)
        up.tick(n + k, nn, 1)
        down.tick(n + AHEAD + k, nn, 1)
        up_gradient(n + k)
    loop(n - AHEAD, lambda k: layer0(k, True))
    loop(n, lambda k: layer0(k, False), n - AHEAD)

    def rest(t):
        up.tick(n + t, nn, 0)
        end_tick(t - (n - AHEAD + 4), 0)
        up.tick(n + t, nn, 1)
    loop(n + up.due[-1][0], rest, n)
    outs = [pltpu.make_async_copy(gf, gf_h, isem.at[0]), pltpu.make_async_copy(dg, dg_h, isem.at[1])]
    for d in outs:
        d.start()
    for d in outs:
        d.wait()


def backward(dy, fgu1, fd0, fd1, a0t, h1, a1, a1t, act, ab, tm, early):
    T, D = dy.shape
    n = fgu1.shape[0]
    F = n * C
    rows, drows = D // 8, F // 8
    nn = n + n
    S = jax.ShapeDtypeStruct
    out = (S(fgu1.shape, bf16), S((nn, rows, W), bf16), S((2, 8, drows, rows), bf16))
    q, w = rows // 4, W

    def V(*shape, dtype=bf16):
        return pltpu.VMEM(shape, dtype)
    return pl.pallas_call(
        functools.partial(backward_kernel, tm, early),
        out_shape=out,
        in_specs=[pl.BlockSpec(memory_space=pl.ANY)] * 10,
        out_specs=[pl.BlockSpec(memory_space=pl.ANY)] * 3,
        input_output_aliases={1: 0},
        scratch_shapes=[
            V(T, D), V(D, T), V(T, D), V(D, T), V(2, T, w, dtype=f32), V(2, D, w), V(2, C, D), V(2, T, C), V(T, w),
            V(SLOTS, D // 2, w), V(D // 2, w), V(SLOTS, D // 2, w), V(2, 2, rows, w), V(SLOTS, 2, rows, w), V(2, rows, w), V(SLOTS, rows, w),
            V(2, 2, q, w), V(SLOTS, 2, q, w), V(SLOTS, 2, q, w, dtype=f32), V(2, q, w), V(SLOTS, q, w), V(nn, rows, w),
            V(SLOTS, C, D // 2), V(2, C, D // 2), V(SLOTS, C, D // 2), V(2, 2, C, rows), V(SLOTS, 2, C, rows), V(2, C, rows), V(SLOTS, C, rows),
            V(2, F, rows), V(2, 2, 2 * drows, rows), V(2, 2 * drows, rows), V(2, 2 * drows, rows), V(2, drows, rows), V(2, 8, drows, rows),
            dma((3,)), dma((4, 2)), dma((7, SLOTS)), dma((7, SLOTS)), dma((3, SLOTS)), dma((3, SLOTS)), dma((5, 2)), dma((5, 2)),
        ] + [dma((n,))] * 6,
        compiler_params=pltpu.CompilerParams(collective_id=1, has_side_effects=True, vmem_limit_bytes=63 * 2**20),
        name="backward",
    )(dy, fgu1, fd0, fd1, a0t, h1, a1, a1t, act, ab)


def adamw(w, m, v, g):
    m = 0.9 * m + 0.1 * g
    v = 0.95 * v + 0.05 * g * g
    step = m * lax.rsqrt(v + 1e-8) + 0.1 * w
    return (w - 0.02 * step).astype(bf16), m, v


def update_kernel(gf, dg, wg, wu, wd, mg, mu, md, vg, vu, vd, *outs):
    def one(part, at, w, m, v, g):
        for o, val in zip(outs[part::3], adamw(wide(w[at]), m[at], v[at], wide(g)), strict=True):
            o[at] = val

    n, _, w = gf.shape
    for k in range(n):
        at = (0, slice(None), pl.ds(k * C, C))
        one(0, at, wg, mg, vg, gf[k, :, :C])
        one(1, at, wu, mu, vu, gf[k, :, C:])
    w = dg.shape[3]
    for j in range(dg.shape[1]):
        one(2, (0, slice(None), pl.ds(j * w, w)), wd, md, vd, dg[0, j])


def update(gf, dg, *arrays):
    wg, wd = arrays[0], arrays[2]
    n = wg.shape[2] // C
    S = jax.ShapeDtypeStruct
    up = pl.BlockSpec((1, wg.shape[1] // PARTS, wg.shape[2]), lambda l, k: (l, k, 0))
    down = pl.BlockSpec((1, wd.shape[1] // PARTS, wd.shape[2]), lambda l, k: (l, k, 0))
    specs = [up, up, down] * 3
    gspec = [pl.BlockSpec((n, gf.shape[1] // PARTS, gf.shape[2]), lambda l, k: (1 - l, k, 0)),
             pl.BlockSpec((1, dg.shape[1], dg.shape[2] // PARTS, dg.shape[3]), lambda l, k: (l, 0, k, 0))]
    return pl.pallas_call(
        update_kernel,
        grid=(2, PARTS),
        out_shape=tuple(S(a.shape, a.dtype) for a in arrays),
        in_specs=gspec + specs,
        out_specs=specs,
        name="update",
    )(gf, dg, *arrays)


PARTS = 4
TM, EARLY = 512, 5


def solution(mesh):
    assert mesh.shape["r"] == 4 and mesh.shape["s"] == 8

    def step(x, dy, *arrays):
        _, fgu1, fd0, fd1, a0t, h1, a1, a1t, act, ab = forward(x[0], *arrays[:3], TM, EARLY)
        _, gf, dg = backward(dy[0], fgu1, fd0, fd1, a0t, h1, a1, a1t, act, ab, TM, EARLY)
        return update(gf, dg, *arrays)

    states, cut = P(("rep", "r", "s"), None, None), P(None, "s", None)
    return jax.shard_map(
        step,
        mesh=mesh,
        in_specs=(states, states) + (cut,) * 9,
        out_specs=(P("rep", "s", None),) * 9,
        check_vma=False,
    )
```
